128 devices in a mesh: ep: 32 (over y, z, core), dp: 4 (over x).
Axes of the slice: x: 4, y: 4, z: 4, core: 2. Of those that a mesh axis runs over, the one named last changes fastest.
Arguments:
- tokens_q: bfloat16 [8192, 3584], P(('dp', 'ep')), parts along dimension 0, may hold values from -448 to 448
- token_scale: float32 [8192, 28], P(('dp', 'ep')), parts along dimension 0, may hold values from 0.003 to 0.03
- residual: bfloat16 [8192, 3584], P(('dp', 'ep')), parts along dimension 0, may hold values from -6 to 6
- expert_ids: int32 [8192, 8], P(('dp', 'ep')), parts along dimension 0, may hold values from 0 to 31, all different within a row; in each aligned block of 64 rows (0 to 63, 64 to 127, ...) at most 32 rows name the same one
- gate_values: float32 [8192, 8], P(('dp', 'ep')), parts along dimension 0, may hold values from 0.1 to 1
- w_gate: bfloat16 [32, 3584, 1024], P('ep'), may hold values from -0.09375 to 0.09375
- w_up: bfloat16 [32, 3584, 1024], P('ep'), may hold values from -0.09375 to 0.09375
- w_down: bfloat16 [32, 1024, 3584], P('ep'), may hold values from -0.1875 to 0.1875
- norm_gain: float32 [3584], replicated, may hold values from 0.5 to 1.5
Outputs:
- new_residual: bfloat16 [8192, 3584], P(('dp', 'ep')), parts along dimension 0
- next_q: bfloat16 [8192, 3584], P(('dp', 'ep')), parts along dimension 0
- next_scale: float32 [8192, 28], P(('dp', 'ep')), parts along dimension 0
The draws below stay inside these ranges and needn't reach their ends.
There are 4 independent parts, one for each index of `dp`. The reference program is written for one: setup_inputs(seed, part) draws one part's arguments, and reference() takes and returns one part's arrays. A program takes and returns all parts, laid end to end along the dimension named above; an argument that names none is the same for every part. Nothing has to cross between parts.
Inputs may be any that keep to these rules, and one draw needn't show every extreme that they name: `expert_ids`: each row names 8 different experts; among the rows of one device no expert is named by more than 32 rows, and in some devices one expert is named by exactly 32.
All inputs are finite; a program needn't handle non-finite values.
Results may differ from the reference program's by a relative error of at most 0.015.
Values may be sent and summed in bfloat16 or wider, within the bound.
A program may use at most 192 MiB of HBM per device.

```python
import math
import jax
import jax.numpy as jnp
import numpy as np
from jax import lax

D = 3584
FF = 1024
QB = 128
TOP = 8
TOK_DEV = 64
EXPERTS = 32
TOKENS = 2048
CAP = 32
N_EP = 32


def steps_of(stream_key, extent, split, smallest, largest):
    def one(dim, shards_of):
        draws = jax.random.uniform(jax.random.fold_in(jax.random.fold_in(stream_key, 6), dim), (shards_of,), jnp.float32, smallest / len(split), largest / len(split))
        return jnp.repeat(jnp.exp(draws), extent[dim] // shards_of).reshape((-1,) + (1,) * (len(extent) - dim - 1))

    gain = one(*split[0])
    for cut in split[1:]:
        gain = gain * one(*cut)
    return gain


def deal_out(rng, own, number, rows, amount, top, bound, skew):
    ranking = jax.random.permutation(rng, amount)
    packed, ordinary = shares(amount, rows * top, bound, skew, True), shares(amount, rows * top, bound, skew, False)
    places = jnp.arange(amount)

    def named(lengths, turn):
        used = int((lengths > 0).sum())
        fixed = max(1, used // 4)
        moved = fixed + (places - fixed + turn * (used - fixed)) % max(1, amount - fixed)
        return jnp.zeros((amount,), jnp.int32).at[ranking[jnp.where(places < fixed, places, moved)]].set(jnp.asarray(lengths, jnp.int32))

    lengths = jnp.where(number % 4 == 0, named(packed, number // 4), named(ordinary, number - number // 4 - 1))
    mixed = jax.random.permutation(jax.random.fold_in(own, 3), amount)
    donor, receiver = mixed[0:amount // 2 * 2:2], mixed[1:amount // 2 * 2:2]
    margin = jnp.minimum(lengths[donor] - 1, bound - lengths[receiver]) // 2
    margin = jnp.where((donor == ranking[0]) | (receiver == ranking[0]) | (lengths[receiver] == 0), 0, jnp.maximum(margin, 0))
    moved = jax.random.randint(jax.random.fold_in(own, 4), (amount // 2,), 0, 1 << 20) % (margin + 1)
    lengths = lengths.at[donor].add(-moved).at[receiver].add(moved)
    members = jnp.searchsorted(jnp.cumsum(lengths), jnp.arange(rows * top), side="right").astype(jnp.int32)
    table = members.reshape(top, rows).T
    table = table[jax.random.permutation(jax.random.fold_in(own, 1), rows)]
    turn = jax.random.randint(jax.random.fold_in(own, 2), (rows, 1), 0, top)
    return jnp.take_along_axis(table, (jnp.arange(top)[None, :] + turn) % top, axis=1)


def shares(count, total, reach, lean, full):
    portions = [(1 << 20) // math.isqrt(standing ** lean) + 1 for standing in range(1, count + 1)]
    largest = reach if full else min(reach, max(-(-total // count), total * portions[0] // sum(portions)))
    least = 1 if total - largest >= count - 1 else 0
    counts, surplus = [largest] + [least] * (count - 1), total - largest - least * (count - 1)
    while surplus > 0:
        free = [i for i in range(1, count) if counts[i] < largest] or [i for i in range(1, count) if counts[i] < reach]
        whole, remaining = sum([portions[i] for i in free]), surplus
        for i in free:
            more = min(reach - counts[i], max(1, remaining * portions[i] // whole), surplus)
            counts[i] = counts[i] + more
            surplus = surplus - more
    return np.array(counts)


def centred(own_key, extent, scale, most, split=(), held_as=jnp.bfloat16):
    values = jax.random.normal(own_key, extent, jnp.float32) * scale
    if len(split) > 0:
        values = steps_of(own_key, extent, split, -0.22, 0.18) * values
    return jnp.clip(values, min=-most, max=most).astype(held_as)


def setup_inputs(seed: int = 0, part: int = 0) -> dict:
    key_list = jax.random.split(jax.random.key(seed), 10)
    own_keys = jax.random.split(jax.random.fold_in(key_list[9], part), 10)
    tokens_q = centred(own_keys[0], (TOKENS, D), 120.0, 448.0, ((0, 32),))
    token_scale = jnp.clip(jnp.exp(math.log(0.03) - 2.3025851 * jax.random.uniform(own_keys[1], (TOKENS, D // QB), jnp.float32) ** steps_of(own_keys[1], (TOKENS, D // QB), ((0, 32),), -0.2, 0.2)), 0.003, 0.03)
    residual = centred(own_keys[2], (TOKENS, D), 1.0, 6.0, ((0, 32),))
    expert_ids_keys = jax.random.split(jax.random.fold_in(own_keys[3], 1), TOKENS // TOK_DEV)
    expert_ids_turns = jax.random.permutation(jax.random.fold_in(own_keys[3], 3), TOKENS // TOK_DEV)
    expert_ids = jax.vmap(lambda own, number: deal_out(jax.random.fold_in(own_keys[3], 2), own, number, TOK_DEV, EXPERTS, TOP, CAP, 2))(expert_ids_keys, expert_ids_turns).reshape((TOKENS, TOP))
    gate_values = jnp.clip(0.1 + 0.9 * jax.random.uniform(own_keys[4], (TOKENS, TOP), jnp.float32) ** steps_of(own_keys[4], (TOKENS, TOP), ((0, 32),), -0.2, 0.2), 0.1, 1.0)
    w_gate = centred(key_list[5], (EXPERTS, D, FF), D ** -0.5, 0.09375, ((0, 32),))
    w_up = centred(key_list[6], (EXPERTS, D, FF), D ** -0.5, 0.09375, ((0, 32),))
    w_down = centred(key_list[7], (EXPERTS, FF, D), FF ** -0.5, 0.1875, ((0, 32),))
    norm_gain = jnp.clip(1.0 + 0.1 * jax.random.normal(key_list[8], (D,), jnp.float32), 0.5, 1.5)
    return dict(tokens_q=tokens_q, token_scale=token_scale, residual=residual, expert_ids=expert_ids, gate_values=gate_values, w_gate=w_gate, w_up=w_up, w_down=w_down, norm_gain=norm_gain)


def slot_of(flat_ids):
    hot = (flat_ids[:, None] == jnp.arange(EXPERTS, dtype=jnp.int32)[None, :]).astype(jnp.int32)
    before = jnp.cumsum(hot, axis=0) - hot
    return lax.optimization_barrier(jnp.sum(before * hot, axis=1)).astype(jnp.int32)

def dequant(payload, scales):
    count = payload.shape[0]
    blocks = payload.astype(jnp.float32).reshape(count, D // QB, QB) * scales[:, :, None]
    return blocks.reshape(count, D).astype(jnp.bfloat16)

def expert_rows(inputs, gates, gate_matrix, up_matrix, down_matrix):
    gate_part = jnp.dot(inputs, gate_matrix, preferred_element_type=jnp.float32)
    up_part = jnp.dot(inputs, up_matrix, preferred_element_type=jnp.float32)
    hidden = (jax.nn.silu(gate_part) * up_part).astype(jnp.bfloat16)
    output = jnp.dot(hidden, down_matrix, preferred_element_type=jnp.float32)
    return (output * gates[:, None]).astype(jnp.bfloat16)

def reference(tokens_q, token_scale, residual, expert_ids, gate_values, w_gate, w_up, w_down, norm_gain):
    inputs = dequant(tokens_q, token_scale)
    per_source = expert_ids.reshape(N_EP, TOK_DEV * TOP)
    slots = jax.vmap(slot_of)(per_source)
    source = jnp.arange(N_EP, dtype=jnp.int32)[:, None] * jnp.ones((1, TOK_DEV * TOP), jnp.int32)
    owner = source * TOK_DEV + (jnp.arange(TOK_DEV * TOP, dtype=jnp.int32) // TOP)[None, :]
    where_slot = source * CAP + slots
    table_token = jnp.zeros((EXPERTS, N_EP * CAP), jnp.int32).at[per_source, where_slot].set(owner)
    table_gate = jnp.zeros((EXPERTS, N_EP * CAP), jnp.float32).at[per_source, where_slot].set(gate_values.reshape(N_EP, TOK_DEV * TOP))

    def one_expert(total, expert):
        rows_index = table_token[expert]
        output = expert_rows(inputs[rows_index], table_gate[expert], w_gate[expert], w_up[expert], w_down[expert])
        return (total.at[rows_index].add(output.astype(jnp.float32)), None)
    total, unused = lax.scan(one_expert, jnp.zeros((TOKENS, D), jnp.float32), jnp.arange(EXPERTS, dtype=jnp.int32))
    mixed = total + residual.astype(jnp.float32)
    new_residual = mixed.astype(jnp.bfloat16)
    meansq = lax.optimization_barrier(jnp.mean(mixed * mixed, axis=-1, keepdims=True))
    normed = mixed * lax.rsqrt(meansq + 1e-06) * norm_gain
    blocks = normed.reshape(TOKENS, D // QB, QB)
    next_scale = (lax.optimization_barrier(jnp.max(jnp.abs(blocks), axis=-1)) + 1e-06) / 448.0
    next_q = (blocks / next_scale[:, :, None]).reshape(TOKENS, D).astype(jnp.bfloat16)
    return (new_residual, next_q, next_scale)
```

```python
import functools

import jax
import jax.numpy as jnp
from jax import lax
from jax.experimental import pallas as pl
from jax.experimental.pallas import tpu as pltpu
from jax.sharding import PartitionSpec as P

MESH = pl.DeviceIdType.MESH
F32 = jnp.float32
BF16 = jnp.bfloat16

BATCHES = (
    ((0, 0), (0, 1), (0, 3), (0, 2)),
    ((3, 0), (1, 0), (3, 1), (1, 3)),
    ((3, 3), (1, 1), (3, 2), (1, 2)),
    ((2, 0), (2, 1), (2, 3), (2, 2)),
)
PLACE = {c: (i, j) for i, b in enumerate(BATCHES) for j, c in enumerate(b)}


def dot(a, b):
    return jnp.dot(a, b, preferred_element_type=F32)


def kernel(
    cap,
    tq, ts, res, ids, gv, gain, wg_hbm, wu_hbm, wd_hbm,
    nr_out, nq_out, ns_out,
    XO, WG, WU, WD, S, RF, RN, QF, Q, XS, H, PF, PB, PT, GS, T, TL, MX,
    w_sem, t_send, t_recv, ag_send, ag_recv, dd_send, dd_recv, s_send, s_recv, r1_send, r1_recv, r2_send, r2_recv,
):
    rows, width = tq.shape
    half = rows // 2
    hidden = wg_hbm.shape[1]
    qb = width // ts.shape[1]
    group = 4 * rows
    slots = 4 * cap
    tile = 512 if width % 512 == 0 else 256
    htile = 256

    ep = lax.axis_index("ep")
    core = ep % 2
    z = (ep // 2) % 4
    y = ep // 8

    def device(da, db, other=False):
        yy = (y + da * (1 - core) + db * core) % 4
        zz = (z + da * core + db * (1 - core)) % 4
        cc = (1 - core) if other else core
        return {"ep": (yy * 4 + zz) * 2 + cc}

    plus_a, minus_a = device(1, 0), device(3, 0)
    plus_b, minus_b = device(0, 1), device(0, 3)
    partner = device(0, 0, True)

    barrier = pltpu.get_barrier_semaphore()

    def greet(k, carry):
        pl.semaphore_signal(barrier, inc=1, device_id={"ep": (ep + k) % 32}, device_id_type=MESH)
        return carry

    lax.fori_loop(1, 32, greet, 0)

    loads = [
        pltpu.make_async_copy(src, dst, w_sem.at[n])
        for n, (src, dst) in enumerate(((wg_hbm, WG), (wu_hbm, WU), (wd_hbm, WD)))
    ]
    for c in loads:
        c.start()

    def xin(db, da, stream=0):
        i, j = PLACE[(db, da)]
        return XO.at[stream, i + 1, pl.ds(rows * j, rows), :]

    def xout(db, da):
        i, j = PLACE[(db, da)]
        return XO.at[0, i, pl.ds(rows * j, rows), :]

    lo = rows * PLACE[(0, 0)][1]
    for n in range(width // qb):
        block = tq[:, n * qb:(n + 1) * qb].astype(F32) * ts[:, n:n + 1]
        XO[0, 1, lo:lo + rows, n * qb:(n + 1) * qb] = block.astype(BF16)

    lane = lax.broadcasted_iota(jnp.int32, (rows, 128), 1)
    dense = jnp.zeros((rows, 128), F32)
    for k in range(ids.shape[1]):
        dense = dense + jnp.where(ids[:, k:k + 1] == lane, gv[:, k:k + 1], 0.0)
    turned = jnp.concatenate([dense, jnp.zeros((128 - rows, 128), F32)], axis=0).T[0:32]
    before = (
        lax.broadcasted_iota(jnp.int32, (128, 128), 0) < lax.broadcasted_iota(jnp.int32, (128, 128), 1)
    ).astype(F32).astype(BF16)
    rank = dot((turned > 0.0).astype(F32).astype(BF16), before)
    for e in range(32):
        TL[e, 0:1, :] = turned[e:e + 1, :]
        TL[e, 1:2, :] = rank[e:e + 1, :]
    PF[...] = jnp.zeros_like(PF)

    pl.semaphore_wait(barrier, 31)

    def remote(src, dst, send, recv, who):
        c = pltpu.make_async_remote_copy(
            src_ref=src, dst_ref=dst, send_sem=send, recv_sem=recv, device_id=who, device_id_type=MESH
        )
        return c

    ag = {}

    def gather_move(key, src, dst, who):
        n = len(ag)
        ag[key] = remote(src, dst, ag_send.at[n], ag_recv.at[n], who)

    top, low = pl.ds(0, half), pl.ds(half, half)
    gather_move(("a", 3), xin(0, 0), xin(0, 3), plus_a)
    gather_move(("a", 1), xin(0, 0), xin(0, 1), minus_a)
    gather_move(("a", "2t"), xin(0, 3).at[top, :], xin(0, 2).at[top, :], plus_a)
    gather_move(("a", "2l"), xin(0, 1).at[low, :], xin(0, 2).at[low, :], minus_a)
    for da in range(4):
        gather_move((3, da), xin(0, da), xin(3, da), plus_b)
        gather_move((1, da), xin(0, da), xin(1, da), minus_b)
    for da in (0, 1):
        gather_move((2, da), xin(3, da), xin(2, da), plus_b)
    for da in (3, 2):
        gather_move((2, da), xin(1, da), xin(2, da), minus_b)
    dd = {}
    for c, (i, j) in PLACE.items():
        n = 4 * i + j
        dd[c] = remote(xin(*c), xin(*c, stream=1), dd_send.at[n], dd_recv.at[n], partner)

    ag[("a", 3)].start()
    ag[("a", 1)].start()
    ag[(3, 0)].start()
    ag[(1, 0)].start()
    dd[(0, 0)].start()

    tables = []
    for s in range(2):
        for (db, da), (i, j) in PLACE.items():
            n = 16 * s + 4 * i + j
            if n == 0:
                continue
            who = device(4 - da, 4 - db, s == 1)
            c = remote(TL.at[who["ep"]], T.at[n], t_send.at[n], t_recv.at[n], who)
            c.start()
            tables.append(c)
    T[0] = TL[ep]

    ag[("a", 3)].wait_recv()
    ag[("a", "2t")].start()
    ag[(3, 3)].start()
    ag[(1, 3)].start()
    dd[(0, 3)].start()
    ag[("a", 1)].wait_recv()
    ag[("a", "2l")].start()
    ag[(3, 1)].start()
    ag[(1, 1)].start()
    dd[(0, 1)].start()
    ag[("a", "2t")].wait_recv()
    ag[("a", "2l")].wait_recv()
    ag[(3, 2)].start()
    ag[(1, 2)].start()
    dd[(0, 2)].start()
    for c in tables:
        c.wait_recv()

    def arrived(db, da):
        ag[(db, da)].wait_recv()
        dd[(db, da)].start()
        if (db == 3 and da in (0, 1)) or (db == 1 and da in (3, 2)):
            ag[(2, da)].start()

    arrived(3, 0)
    arrived(1, 0)

    def tables_of(i):
        slot = lax.broadcasted_iota(jnp.int32, (cap, 128), 0).astype(F32)
        for s in range(2):
            for j in range(4):
                t = T[16 * s + 4 * i + j]
                gate, place = t[0:1, :], t[1:2, :]
                pick = jnp.where((slot == place) & (gate > 0.0), 1.0, 0.0)
                weight = jnp.sum(pick * gate, axis=1, keepdims=True)
                GS[slots * s + cap * j:slots * s + cap * (j + 1), :] = jnp.broadcast_to(weight, (cap, 128))
                if rows == 64 and j % 2 == 1:
                    pick = pltpu.roll(pick, 64, 1)
                block = 128 * (rows * j // 128)
                PF[s, cap * j:cap * (j + 1), block:block + 128] = pick
            PB[s] = PF[s].astype(BF16)
            PT[s] = PF[s].T.astype(BF16)

    def gather_rows(i, s):
        def step(n, carry):
            cols = pl.ds(pl.multiple_of(n * tile, tile), tile)
            XS[slots * s:slots * (s + 1), cols] = dot(PB[s], XO[s, i + 1, :, cols]).astype(BF16)
            return carry

        lax.fori_loop(0, width // tile, step, 0)

    def gate_up():
        def step(n, carry):
            cols = pl.ds(pl.multiple_of(n * htile, htile), htile)
            g = dot(XS[...], WG[:, cols])
            u = dot(XS[...], WU[:, cols])
            H[:, cols] = (g / (1.0 + jnp.exp(-g)) * u).astype(BF16)
            return carry

        lax.fori_loop(0, hidden // htile, step, 0)

    def down(i):
        def step(n, carry):
            cols = pl.ds(pl.multiple_of(n * tile, tile), tile)
            part = (dot(H[...], WD[:, cols]) * GS[:, 0:1]).astype(BF16)
            for s in range(2):
                XO[s, i, :, cols] = dot(PT[s], part[slots * s:slots * (s + 1)]).astype(BF16)
            return carry

        lax.fori_loop(0, width // tile, step, 0)

    step_rows = 16

    def add_into(dst, src):
        def step(n, carry):
            r = pl.ds(pl.multiple_of(n * step_rows, step_rows), step_rows)
            dst[r, :] = (dst[r, :].astype(F32) + src[r, :].astype(F32)).astype(BF16)
            return carry

        lax.fori_loop(0, dst.shape[0] // step_rows, step, 0)

    swap = [
        remote(XO.at[1, i], S.at[i], s_send.at[i], s_recv.at[i], partner) for i in range(4)
    ]

    def merge(i):
        swap[i].wait_recv()
        add_into(XO.at[0, i], S.at[i])

    r1 = {}

    def r1_move(key, src, dst, who):
        n = len(r1)
        r1[key] = remote(src, dst, r1_send.at[n], r1_recv.at[n], who)

    for n, da in enumerate((1, 0)):
        r1_move(("f", 0, n), xout(2, da), RF.at[0, n], plus_b)
    for n, da in enumerate((2, 3)):
        r1_move(("f", 1, n), xout(2, da), RF.at[1, n], minus_b)
    for da in range(4):
        r1_move(("n", 0, da), xout(1, da), RN.at[0, da], plus_b)
        r1_move(("n", 1, da), xout(3, da), RN.at[1, da], minus_b)

    def sent(i):
        for (db, da) in BATCHES[i]:
            dd[(db, da)].wait_send()
        if i == 0:
            for key in (("a", 3), ("a", 1), ("a", "2t"), ("a", "2l")):
                ag[key].wait_send()
            for da in range(4):
                ag[(3, da)].wait_send()
                ag[(1, da)].wait_send()
        for (db, da) in BATCHES[i]:
            if (db == 3 and da in (0, 1)) or (db == 1 and da in (3, 2)):
                ag[(2, da)].wait_send()

    for c in loads[:2]:
        c.wait()

    for i in range(4):
        tables_of(i)
        gather_rows(i, 0)
        for c in BATCHES[i]:
            dd[c].wait_recv()
        gather_rows(i, 1)
        gate_up()
        if i == 0:
            loads[2].wait()
            arrived(3, 1)
            arrived(1, 3)
        elif i == 1:
            arrived(3, 3)
            arrived(1, 1)
            merge(0)
        elif i == 2:
            merge(1)
            r1[("n", 0, 3)].start()
            r1[("n", 1, 1)].start()
            r1[("n", 1, 0)].start()
            arrived(2, 0)
            arrived(2, 3)
        elif i == 3:
            merge(2)
            r1[("n", 0, 2)].start()
        if i > 0:
            sent(i - 1)
        down(i)
        swap[i].start()
        if i == 1:
            arrived(3, 2)
            arrived(1, 2)
        elif i == 2:
            arrived(2, 1)
            arrived(2, 2)
    merge(3)
    for key in (("f", 0, 0), ("f", 1, 0), ("f", 0, 1), ("f", 1, 1)):
        r1[key].start()

    for n in range(2):
        da = (1, 0)[n]
        r1[("f", 0, n)].wait_recv()
        add_into(xout(1, da), RF.at[0, n])
        r1[("n", 0, da)].start()
        da = (2, 3)[n]
        r1[("f", 1, n)].wait_recv()
        add_into(xout(3, da), RF.at[1, n])
        r1[("n", 1, da)].start()

    def collect(da):
        r1[("n", 0, da)].wait_recv()
        r1[("n", 1, da)].wait_recv()
        dst, p, m = xout(0, da), RN.at[0, da], RN.at[1, da]

        def step(n, carry):
            r = pl.ds(pl.multiple_of(n * step_rows, step_rows), step_rows)
            dst[r, :] = (dst[r, :].astype(F32) + p[r, :].astype(F32) + m[r, :].astype(F32)).astype(BF16)
            return carry

        lax.fori_loop(0, rows // step_rows, step, 0)

    r2 = [
        remote(xout(0, 2).at[top, :], QF.at[0], r2_send.at[0], r2_recv.at[0], plus_a),
        remote(xout(0, 2).at[low, :], QF.at[1], r2_send.at[1], r2_recv.at[1], minus_a),
        remote(xout(0, 1).at[low, :], Q.at[0].at[low, :], r2_send.at[2], r2_recv.at[2], plus_a),
        remote(xout(0, 3).at[top, :], Q.at[1].at[top, :], r2_send.at[3], r2_recv.at[3], minus_a),
        remote(xout(0, 1).at[top, :], Q.at[0].at[top, :], r2_send.at[4], r2_recv.at[4], plus_a),
        remote(xout(0, 3).at[low, :], Q.at[1].at[low, :], r2_send.at[5], r2_recv.at[5], minus_a),
    ]
    collect(2)
    r2[0].start()
    r2[1].start()
    collect(1)
    r2[2].start()
    collect(3)
    r2[3].start()
    r2[0].wait_recv()
    add_into(xout(0, 1).at[top, :], QF.at[0])
    r2[4].start()
    r2[1].wait_recv()
    add_into(xout(0, 3).at[low, :], QF.at[1])
    r2[5].start()

    r1[("n", 0, 0)].wait_recv()
    r1[("n", 1, 0)].wait_recv()
    mine = xout(0, 0)

    def start_sum(n, carry):
        r = pl.ds(pl.multiple_of(n * step_rows, step_rows), step_rows)
        MX[r, :] = (
            res[r, :].astype(F32)
            + mine[r, :].astype(F32)
            + RN[0, 0, r, :].astype(F32)
            + RN[1, 0, r, :].astype(F32)
        )
        return carry

    lax.fori_loop(0, rows // step_rows, start_sum, 0)
    for n in (2, 3, 4, 5):
        r2[n].wait_recv()

    def finish(n, carry):
        r = pl.ds(pl.multiple_of(n * step_rows, step_rows), step_rows)
        mixed = MX[r, :] + Q[0, r, :].astype(F32) + Q[1, r, :].astype(F32)
        nr_out[r, :] = mixed.astype(BF16)
        meansq = jnp.mean(mixed * mixed, axis=-1, keepdims=True)
        normed = mixed * lax.rsqrt(meansq + 1e-06) * gain[...]
        lanes = lax.broadcasted_iota(jnp.int32, (step_rows, 128), 1)
        scales = jnp.zeros((step_rows, 128), F32)
        for b in range(width // qb):
            block = normed[:, b * qb:(b + 1) * qb]
            scale = (jnp.max(jnp.abs(block), axis=-1, keepdims=True) + 1e-06) / 448.0
            nq_out[r, b * qb:(b + 1) * qb] = (block / scale).astype(BF16)
            scales = jnp.where(lanes == b, scale, scales)
        ns_out[r, :] = scales[:, 0:width // qb]
        return carry

    lax.fori_loop(0, rows // step_rows, finish, 0)

    for i in (3,):
        sent(i)
    for c in swap:
        c.wait_send()
    for c in tables:
        c.wait_send()
    for c in r1.values():
        c.wait_send()
    for c in r2:
        c.wait_send()


def per_device(
    tokens_q, token_scale, residual, expert_ids, gate_values, w_gate, w_up, w_down, norm_gain
):
    rows, width = tokens_q.shape
    hidden = w_gate.shape[2]
    cap = rows // 2
    vmem = pl.BlockSpec(memory_space=pltpu.VMEM)
    hbm = pl.BlockSpec(memory_space=pl.ANY)
    dma = pltpu.SemaphoreType.DMA
    return pl.pallas_call(
        functools.partial(kernel, cap),
        out_shape=(
            jax.ShapeDtypeStruct((rows, width), BF16),
            jax.ShapeDtypeStruct((rows, width), BF16),
            jax.ShapeDtypeStruct(token_scale.shape, F32),
        ),
        in_specs=[vmem] * 6 + [hbm] * 3,
        out_specs=(vmem, vmem, vmem),
        scratch_shapes=[
            pltpu.VMEM((2, 5, 4 * rows, width), BF16),
            pltpu.VMEM((width, hidden), BF16),
            pltpu.VMEM((width, hidden), BF16),
            pltpu.VMEM((hidden, width), BF16),
            pltpu.VMEM((4, 4 * rows, width), BF16),
            pltpu.VMEM((2, 2, rows, width), BF16),
            pltpu.VMEM((2, 4, rows, width), BF16),
            pltpu.VMEM((2, rows // 2, width), BF16),
            pltpu.VMEM((2, rows, width), BF16),
            pltpu.VMEM((8 * cap, width), BF16),
            pltpu.VMEM((8 * cap, hidden), BF16),
            pltpu.VMEM((2, 4 * cap, 4 * rows), F32),
            pltpu.VMEM((2, 4 * cap, 4 * rows), BF16),
            pltpu.VMEM((2, 4 * rows, 4 * cap), BF16),
            pltpu.VMEM((8 * cap, 128), F32),
            pltpu.VMEM((32, 2, 128), F32),
            pltpu.VMEM((32, 2, 128), F32),
            pltpu.VMEM((rows, width), F32),
            dma((3,)), dma((32,)), dma((32,)), dma((16,)), dma((16,)), dma((16,)), dma((16,)),
            dma((4,)), dma((4,)), dma((12,)), dma((12,)), dma((6,)), dma((6,)),
        ],
        compiler_params=pltpu.CompilerParams(
            collective_id=0, has_side_effects=True, vmem_limit_bytes=67043328
        ),
    )(
        tokens_q, token_scale, residual, expert_ids, gate_values, norm_gain.reshape(1, width),
        w_gate[0], w_up[0], w_down[0],
    )


def solution(mesh):
    rows = P(("dp", "ep"), None)
    weight = P("ep", None, None)
    return jax.shard_map(
        per_device,
        mesh=mesh,
        in_specs=(rows, rows, rows, rows, rows, weight, weight, weight, P()),
        out_specs=(rows, rows, rows),
        check_vma=False,
    )
```

```python
import functools

import jax
import jax.numpy as jnp
from jax import lax
from jax.experimental import pallas as pl
from jax.experimental.pallas import tpu as pltpu
from jax.sharding import PartitionSpec as P

MESH = pl.DeviceIdType.MESH
F32 = jnp.float32
BF16 = jnp.bfloat16

BATCHES = (
    ((0, 0), (0, 1), (0, 3), (0, 2)),
    ((1, 0), (3, 1), (1, 3), (2, 0)),
    ((2, 2), (2, 3), (2, 1), (3, 0)),
    ((3, 2), (1, 1), (1, 2), (3, 3)),
)
HOLD = (0, 1, 3, 4)
PLACE = {c: (i, j) for i, b in enumerate(BATCHES) for j, c in enumerate(b)}


def tile_of(width):
    return 896 if width % 896 == 0 else 256


def dot(a, b):
    return jnp.dot(a, b, preferred_element_type=F32)


def kernel(
    cap,
    tq, ts, res, ids, gv, wg_hbm, wu_hbm, wd_hbm,
    mixed_out,
    XO, WG, WU, WD, S, RF, RN, QF, Q, H, GU, PV, PF, PB, PT, GS, T, TL, SQ,
    w_sem, t_send, t_recv, ag_send, ag_recv, dd_send, dd_recv, s_send, s_recv, r1_send, r1_recv, r2_send, r2_recv,
):
    rows, width = tq.shape
    half = rows // 2
    hidden = wg_hbm.shape[1]
    qb = width // ts.shape[0]
    group = 4 * rows
    slots = 4 * cap
    tile = tile_of(width)
    htile = 256

    ep = lax.axis_index("ep")
    core = ep % 2
    z = (ep // 2) % 4
    y = ep // 8

    def device(da, db, other=False):
        yy = (y + da * (1 - core) + db * core) % 4
        zz = (z + da * core + db * (1 - core)) % 4
        cc = (1 - core) if other else core
        return {"ep": (yy * 4 + zz) * 2 + cc}

    plus_a, minus_a = device(1, 0), device(3, 0)
    plus_b, minus_b = device(0, 1), device(0, 3)
    partner = device(0, 0, True)

    barrier = pltpu.get_barrier_semaphore()

    def greet(k, carry):
        pl.semaphore_signal(barrier, inc=1, device_id={"ep": (ep + k) % 32}, device_id_type=MESH)
        return carry

    lax.fori_loop(1, 32, greet, 0)

    loads = [
        pltpu.make_async_copy(src, dst, w_sem.at[n])
        for n, (src, dst) in enumerate(((wg_hbm, WG), (wu_hbm, WU), (wd_hbm, WD)))
    ]
    for c in loads:
        c.start()

    def xin(db, da, stream=0):
        i, j = PLACE[(db, da)]
        return XO.at[stream, i + 2, pl.ds(rows * j, rows), :]

    def xout(db, da):
        i, j = PLACE[(db, da)]
        return XO.at[0, i, pl.ds(rows * j, rows), :]

    lo = rows * PLACE[(0, 0)][1]
    SQ[...] = jnp.zeros_like(SQ)
    SQ[0:width // qb, 0:rows] = ts[...]
    scales = SQ[...].T[0:rows]
    for n in range(width // qb):
        block = tq[:, n * qb:(n + 1) * qb].astype(F32) * scales[:, n:n + 1]
        XO[0, 2, lo:lo + rows, n * qb:(n + 1) * qb] = block.astype(BF16)

    expert = lax.broadcasted_iota(jnp.int32, (32, rows), 0)
    gates = jnp.zeros((32, rows), F32)
    for k in range(ids.shape[0]):
        gates = gates + jnp.where(ids[k:k + 1, :] == expert, gv[k:k + 1, :], 0.0)
    before = (
        lax.broadcasted_iota(jnp.int32, (rows, rows), 0) < lax.broadcasted_iota(jnp.int32, (rows, rows), 1)
    ).astype(F32).astype(BF16)
    rank = dot((gates > 0.0).astype(F32).astype(BF16), before)
    TL[...] = jnp.zeros_like(TL)
    for e in range(32):
        TL[e, 0:1, 0:rows] = gates[e:e + 1, :]
        TL[e, 1:2, 0:rows] = rank[e:e + 1, :]
    PF[...] = jnp.zeros_like(PF)

    pl.semaphore_wait(barrier, 31)

    def remote(src, dst, send, recv, who):
        c = pltpu.make_async_remote_copy(
            src_ref=src, dst_ref=dst, send_sem=send, recv_sem=recv, device_id=who, device_id_type=MESH
        )
        return c

    ag = {}
    leaving = {i: [] for i in range(4)}

    def gather_move(key, src_place, src, dst, who):
        n = len(ag)
        ag[key] = remote(src, dst, ag_send.at[n], ag_recv.at[n], who)
        leaving[PLACE[src_place][0]].append(ag[key])

    top, low = pl.ds(0, half), pl.ds(half, half)
    for name, part in (("t", top), ("l", low)):
        gather_move(("a", "3" + name), (0, 0), xin(0, 0).at[part, :], xin(0, 3).at[part, :], plus_a)
        gather_move(("a", "1" + name), (0, 0), xin(0, 0).at[part, :], xin(0, 1).at[part, :], minus_a)
    gather_move(("a", "2t"), (0, 3), xin(0, 3).at[top, :], xin(0, 2).at[top, :], plus_a)
    gather_move(("a", "2l"), (0, 1), xin(0, 1).at[low, :], xin(0, 2).at[low, :], minus_a)
    for da in range(4):
        gather_move((3, da), (0, da), xin(0, da), xin(3, da), plus_b)
        gather_move((1, da), (0, da), xin(0, da), xin(1, da), minus_b)
    for da in (0, 1):
        gather_move((2, da), (3, da), xin(3, da), xin(2, da), plus_b)
    for da in (3, 2):
        gather_move((2, da), (1, da), xin(1, da), xin(2, da), minus_b)
    dd = {}
    for c, (i, j) in PLACE.items():
        n = 4 * i + j
        dd[c] = remote(xin(*c), xin(*c, stream=1), dd_send.at[n], dd_recv.at[n], partner)
        leaving[i].append(dd[c])

    ag[("a", "3t")].start()
    ag[("a", "1l")].start()
    ag[("a", "3l")].start()
    ag[("a", "1t")].start()
    dd[(0, 0)].start()

    tables = []
    for s in range(2):
        for (db, da), (i, j) in PLACE.items():
            n = 16 * s + 4 * i + j
            if n == 0:
                continue
            who = device(4 - da, 4 - db, s == 1)
            c = remote(TL.at[who["ep"]], T.at[n], t_send.at[n], t_recv.at[n], who)
            c.start()
            tables.append(c)
    T[0] = TL[ep]

    def arrived(db, da):
        ag[(db, da)].wait_recv()
        if (db == 3 and da in (0, 1)) or (db == 1 and da in (3, 2)):
            ag[(2, da)].start()
        dd[(db, da)].start()

    def tables_of(i):
        slot = lax.broadcasted_iota(jnp.int32, (cap, 128), 0).astype(F32)
        for s in range(2):
            for j in range(4):
                t = T[16 * s + 4 * i + j]
                gate, place = t[0:1, :], t[1:2, :]
                pick = jnp.where((slot == place) & (gate > 0.0), 1.0, 0.0)
                weight = jnp.sum(pick * gate, axis=1, keepdims=True)
                GS[i, slots * s + cap * j:slots * s + cap * (j + 1), :] = jnp.broadcast_to(weight, (cap, 128))
                if rows == 64 and j % 2 == 1:
                    pick = pltpu.roll(pick, 64, 1)
                block = 128 * (rows * j // 128)
                PF[s, cap * j:cap * (j + 1), block:block + 128] = pick
            PB[i, s] = PF[s].astype(BF16)
            PT[i, s] = PF[s].T.astype(BF16)

    ag[("a", "3t")].wait_recv()
    ag[("a", "2t")].start()
    ag[("a", "1l")].wait_recv()
    ag[("a", "2l")].start()
    ag[(3, 0)].start()
    ag[(1, 0)].start()
    for c in tables:
        c.wait_recv()
    for i in range(2):
        tables_of(i)
    ag[("a", "1t")].wait_recv()
    ag[(3, 1)].start()
    ag[("a", "3l")].wait_recv()
    ag[(1, 3)].start()
    dd[(0, 1)].start()
    dd[(0, 3)].start()
    ag[("a", "2t")].wait_recv()
    ag[("a", "2l")].wait_recv()
    ag[(1, 2)].start()
    dd[(0, 2)].start()
    for i in range(2, 4):
        tables_of(i)
    arrived(3, 0)
    arrived(1, 0)
    ag[(3, 3)].start()

    wide = width // 2 if width % 256 == 0 else width

    def gather_rows(i, s):
        for n in range(width // wide):
            cols = slice(n * wide, (n + 1) * wide)
            XO[0, HOLD[i], slots * s:slots * (s + 1), cols] = dot(PB[i, s], XO[s, i + 2, :, cols]).astype(BF16)

    def gate_up(i):
        def products(n):
            cols = pl.ds(pl.multiple_of(n * htile, htile), htile)
            GU[n % 2, 0] = dot(XO[0, HOLD[i]], WG[:, cols])
            GU[n % 2, 1] = dot(XO[0, HOLD[i]], WU[:, cols])

        def activate(n):
            cols = pl.ds(pl.multiple_of(n * htile, htile), htile)
            g = GU[n % 2, 0]
            H[:, cols] = (g / (1.0 + jnp.exp(-g)) * GU[n % 2, 1]).astype(BF16)

        def step(n, carry):
            activate(n - 1)
            products(n)
            return carry

        products(0)
        lax.fori_loop(1, hidden // htile, step, 0)
        activate(hidden // htile - 1)

    def down(i):
        def part(n):
            cols = pl.ds(pl.multiple_of(n * tile, tile), tile)
            PV[n % 2] = (dot(H[...], WD[:, cols]) * GS[i, :, 0:1]).astype(BF16)

        def spread(n):
            cols = pl.ds(pl.multiple_of(n * tile, tile), tile)
            for s in range(2):
                XO[s, i, :, cols] = dot(PT[i, s], PV[n % 2, slots * s:slots * (s + 1)]).astype(BF16)

        def step(n, carry):
            spread(n - 1)
            part(n)
            return carry

        part(0)
        lax.fori_loop(1, width // tile, step, 0)
        spread(width // tile - 1)

    step_rows = 16

    def add_into(dst, *sources):
        def step(n, carry):
            r = pl.ds(pl.multiple_of(n * step_rows, step_rows), step_rows)
            total = dst[r, :].astype(F32)
            for src in sources:
                total = total + src[r, :].astype(F32)
            dst[r, :] = total.astype(BF16)
            return carry

        lax.fori_loop(0, dst.shape[0] // step_rows, step, 0)

    def part_of(db, da):
        i, j = PLACE[(db, da)]
        return S.at[i, pl.ds(rows * j, rows), :]

    swap = {}
    for c, (i, j) in PLACE.items():
        n = 4 * i + j
        src = XO.at[1, i, pl.ds(rows * j, rows), :]
        swap[c] = remote(src, part_of(*c), s_send.at[n], s_recv.at[n], partner)

    def merge(db, da, *more):
        swap[(db, da)].wait_recv()
        add_into(xout(db, da), part_of(db, da), *more)

    r1 = {}

    def r1_move(key, src, dst, who):
        n = len(r1)
        r1[key] = remote(src, dst, r1_send.at[n], r1_recv.at[n], who)

    far = ((2, 1), (0, 3))
    for n in range(2):
        r1_move(("f", 0, n), xout(2, far[0][n]), RF.at[0, n], plus_b)
        r1_move(("f", 1, n), xout(2, far[1][n]), RF.at[1, n], minus_b)
    for da in range(4):
        r1_move(("n", 0, da), xout(1, da), RN.at[0, da], plus_b)
        r1_move(("n", 1, da), xout(3, da), RN.at[1, da], minus_b)

    def sent(i):
        for c in leaving[i]:
            c.wait_send()

    def pass_on(sign, n):
        db, da = (1, 3)[sign], far[sign][n]
        r1[("f", sign, n)].wait_recv()
        merge(db, da, RF.at[sign, n])
        r1[("n", sign, da)].start()

    def send_far(sign, n):
        merge(2, far[sign][n])
        r1[("f", sign, n)].start()

    def send_near(sign, da):
        merge((1, 3)[sign], da)
        r1[("n", sign, da)].start()

    for c in loads[:2]:
        c.wait()

    for i in range(4):
        for c in BATCHES[i]:
            dd[c].wait_recv()
        if i > 1:
            sent(i - 1)
        gather_rows(i, 0)
        gather_rows(i, 1)
        gate_up(i)
        if i == 0:
            loads[2].wait()
            arrived(3, 1)
            arrived(1, 3)
            ag[(3, 2)].start()
        elif i == 1:
            arrived(3, 3)
            arrived(2, 3)
        elif i == 2:
            send_near(0, 0)
            send_near(1, 1)
            send_near(0, 3)
            send_far(1, 0)
            arrived(3, 2)
            arrived(1, 1)
        elif i == 3:
            send_far(0, 0)
            send_far(1, 1)
            send_far(0, 1)
            pass_on(1, 0)
        if i == 2:
            sent(0)
        down(i)
        for c in BATCHES[i]:
            swap[c].start()
        if i == 0:
            arrived(1, 2)
            ag[(1, 1)].start()
            arrived(2, 0)
        elif i == 1:
            arrived(2, 1)
            arrived(2, 2)
    send_near(1, 2)
    pass_on(0, 0)
    pass_on(1, 1)
    pass_on(0, 1)

    def collect(da):
        r1[("n", 0, da)].wait_recv()
        r1[("n", 1, da)].wait_recv()
        merge(0, da, RN.at[0, da], RN.at[1, da])

    r2 = [
        remote(xout(0, 2).at[top, :], QF.at[0], r2_send.at[0], r2_recv.at[0], plus_a),
        remote(xout(0, 2).at[low, :], QF.at[1], r2_send.at[1], r2_recv.at[1], minus_a),
        remote(xout(0, 1).at[low, :], Q.at[0].at[low, :], r2_send.at[2], r2_recv.at[2], plus_a),
        remote(xout(0, 3).at[top, :], Q.at[1].at[top, :], r2_send.at[3], r2_recv.at[3], minus_a),
        remote(xout(0, 1).at[top, :], Q.at[0].at[top, :], r2_send.at[4], r2_recv.at[4], plus_a),
        remote(xout(0, 3).at[low, :], Q.at[1].at[low, :], r2_send.at[5], r2_recv.at[5], minus_a),
    ]
    collect(2)
    r2[0].start()
    r2[1].start()
    collect(1)
    r2[2].start()
    collect(3)
    r2[3].start()
    r2[0].wait_recv()
    add_into(xout(0, 1).at[top, :], QF.at[0])
    r2[4].start()
    r2[1].wait_recv()
    add_into(xout(0, 3).at[low, :], QF.at[1])
    r2[5].start()

    r1[("n", 0, 0)].wait_recv()
    r1[("n", 1, 0)].wait_recv()
    mine, partners = xout(0, 0), part_of(0, 0)
    swap[(0, 0)].wait_recv()

    def start_sum(n, carry):
        r = pl.ds(pl.multiple_of(n * step_rows, step_rows), step_rows)
        mixed_out[r, :] = (
            res[r, :].astype(F32)
            + mine[r, :].astype(F32)
            + partners[r, :].astype(F32)
            + RN[0, 0, r, :].astype(F32)
            + RN[1, 0, r, :].astype(F32)
        )
        return carry

    lax.fori_loop(0, rows // step_rows, start_sum, 0)
    for n in (2, 3, 4, 5):
        r2[n].wait_recv()

    def finish(n, carry):
        r = pl.ds(pl.multiple_of(n * step_rows, step_rows), step_rows)
        mixed_out[r, :] = mixed_out[r, :] + Q[0, r, :].astype(F32) + Q[1, r, :].astype(F32)
        return carry

    lax.fori_loop(0, rows // step_rows, finish, 0)

    sent(3)
    for c in swap.values():
        c.wait_send()
    for c in tables:
        c.wait_send()
    for c in r1.values():
        c.wait_send()
    for c in r2:
        c.wait_send()


def norm_kernel(mixed_ref, gain, nr_out, nq_out, ns_out, SQ):
    rows, width = mixed_ref.shape
    qb = width // ns_out.shape[0]
    step_rows = 16
    SQ[...] = jnp.zeros_like(SQ)

    def step(n, carry):
        r = pl.ds(pl.multiple_of(n * step_rows, step_rows), step_rows)
        mixed = mixed_ref[r, :]
        nr_out[r, :] = mixed.astype(BF16)
        scaled = lax.rsqrt(jnp.mean(mixed * mixed, axis=-1, keepdims=True) + 1e-06)
        lanes = lax.broadcasted_iota(jnp.int32, (step_rows, 128), 1)
        scales = jnp.zeros((step_rows, 128), F32)
        for b in range(width // qb):
            block = mixed[:, b * qb:(b + 1) * qb] * scaled * gain[b:b + 1, :]
            scale = (jnp.max(jnp.abs(block), axis=-1, keepdims=True) + 1e-06) / 448.0
            nq_out[r, b * qb:(b + 1) * qb] = (block / scale).astype(BF16)
            scales = jnp.where(lanes == b, scale, scales)
        SQ[r, :] = scales
        return carry

    lax.fori_loop(0, rows // step_rows, step, 0)
    ns_out[...] = SQ[...].T[0:width // qb, 0:rows]


def per_device(
    tokens_q, token_scale, residual, expert_ids, gate_values, w_gate, w_up, w_down, norm_gain
):
    rows, width = tokens_q.shape
    blocks = token_scale.shape[1]
    hidden = w_gate.shape[2]
    cap = rows // 2
    vmem = pl.BlockSpec(memory_space=pltpu.VMEM)
    hbm = pl.BlockSpec(memory_space=pl.ANY)
    dma = pltpu.SemaphoreType.DMA
    mixed = pl.pallas_call(
        functools.partial(kernel, cap),
        out_shape=jax.ShapeDtypeStruct((rows, width), F32),
        in_specs=[vmem] * 5 + [hbm] * 3,
        out_specs=vmem,
        scratch_shapes=[
            pltpu.VMEM((2, 6, 4 * rows, width), BF16),
            pltpu.VMEM((width, hidden), BF16),
            pltpu.VMEM((width, hidden), BF16),
            pltpu.VMEM((hidden, width), BF16),
            pltpu.VMEM((4, 4 * rows, width), BF16),
            pltpu.VMEM((2, 2, rows, width), BF16),
            pltpu.VMEM((2, 4, rows, width), BF16),
            pltpu.VMEM((2, rows // 2, width), BF16),
            pltpu.VMEM((2, rows, width), BF16),
            pltpu.VMEM((8 * cap, hidden), BF16),
            pltpu.VMEM((2, 2, 8 * cap, 256), F32),
            pltpu.VMEM((2, 8 * cap, tile_of(width)), BF16),
            pltpu.VMEM((2, 4 * cap, 4 * rows), F32),
            pltpu.VMEM((4, 2, 4 * cap, 4 * rows), BF16),
            pltpu.VMEM((4, 2, 4 * rows, 4 * cap), BF16),
            pltpu.VMEM((4, 8 * cap, 128), F32),
            pltpu.VMEM((32, 2, 128), F32),
            pltpu.VMEM((32, 2, 128), F32),
            pltpu.VMEM((128, 128), F32),
            dma((3,)), dma((32,)), dma((32,)), dma((18,)), dma((18,)), dma((16,)), dma((16,)),
            dma((16,)), dma((16,)), dma((12,)), dma((12,)), dma((6,)), dma((6,)),
        ],
        compiler_params=pltpu.CompilerParams(
            collective_id=0, has_side_effects=True, vmem_limit_bytes=67043328
        ),
    )(
        tokens_q, token_scale.T, residual, expert_ids.T, gate_values.T,
        w_gate[0], w_up[0], w_down[0],
    )
    new_residual, next_q, next_scale = pl.pallas_call(
        norm_kernel,
        out_shape=(
            jax.ShapeDtypeStruct((rows, width), BF16),
            jax.ShapeDtypeStruct((rows, width), BF16),
            jax.ShapeDtypeStruct((blocks, rows), F32),
        ),
        in_specs=[vmem] * 2,
        out_specs=(vmem, vmem, vmem),
        scratch_shapes=[pltpu.VMEM((128, 128), F32)],
    )(mixed, norm_gain.reshape(blocks, width // blocks))
    return new_residual, next_q, next_scale.T


def solution(mesh):
    rows = P(("dp", "ep"), None)
    weight = P("ep", None, None)
    return jax.shard_map(
        per_device,
        mesh=mesh,
        in_specs=(rows, rows, rows, rows, rows, weight, weight, weight, P()),
        out_specs=(rows, rows, rows),
        check_vma=False,
    )
```

```python
import functools

import jax
import jax.numpy as jnp
from jax import lax
from jax.experimental import pallas as pl
from jax.experimental.pallas import tpu as pltpu
from jax.sharding import PartitionSpec as P

MESH = pl.DeviceIdType.MESH
F32 = jnp.float32
BF16 = jnp.bfloat16

BATCHES = (
    ((0, 0), (0, 1), (0, 3), (0, 2)),
    ((2, 0), (1, 0), (3, 1), (1, 3)),
    ((2, 2), (2, 3), (2, 1), (3, 0)),
    ((3, 2), (1, 1), (1, 2), (3, 3)),
)
HOLD = (0, 1, 3, 4)
PLACE = {c: (i, j) for i, b in enumerate(BATCHES) for j, c in enumerate(b)}


def tile_of(width):
    return 896 if width % 896 == 0 else 256


def dot(a, b):
    return jnp.dot(a, b, preferred_element_type=F32)


def kernel(
    cap,
    tq, ts, res, ids, gv, wg_hbm, wu_hbm, wd_hbm,
    mixed_out,
    XO, WG, WU, WD, S, RF, RN, QF, Q, H, GU, PV, PF, PB, PT, GS, T, TL, SQ,
    w_sem, t_send, t_recv, ag_send, ag_recv, dd_send, dd_recv, s_send, s_recv, r1_send, r1_recv, r2_send, r2_recv,
):
    rows, width = tq.shape
    half = rows // 2
    hidden = wg_hbm.shape[1]
    qb = width // ts.shape[0]
    group = 4 * rows
    slots = 4 * cap
    tile = tile_of(width)
    htile = 256

    ep = lax.axis_index("ep")
    core = ep % 2
    z = (ep // 2) % 4
    y = ep // 8

    def device(da, db, other=False):
        yy = (y + da * (1 - core) + db * core) % 4
        zz = (z + da * core + db * (1 - core)) % 4
        cc = (1 - core) if other else core
        return {"ep": (yy * 4 + zz) * 2 + cc}

    plus_a, minus_a = device(1, 0), device(3, 0)
    plus_b, minus_b = device(0, 1), device(0, 3)
    partner = device(0, 0, True)

    barrier = pltpu.get_barrier_semaphore()

    def greet(k, carry):
        pl.semaphore_signal(barrier, inc=1, device_id={"ep": (ep + k) % 32}, device_id_type=MESH)
        return carry

    lax.fori_loop(1, 32, greet, 0)

    loads = [
        pltpu.make_async_copy(src, dst, w_sem.at[n])
        for n, (src, dst) in enumerate(((wg_hbm, WG), (wu_hbm, WU), (wd_hbm, WD)))
    ]
    for c in loads:
        c.start()

    def xin(db, da, stream=0):
        i, j = PLACE[(db, da)]
        return XO.at[stream, i + 2, pl.ds(rows * j, rows), :]

    def xout(db, da):
        i, j = PLACE[(db, da)]
        return XO.at[0, i, pl.ds(rows * j, rows), :]

    lo = rows * PLACE[(0, 0)][1]
    SQ[...] = jnp.zeros_like(SQ)
    SQ[0:width // qb, 0:rows] = ts[...]
    scales = SQ[...].T[0:rows]
    for n in range(width // qb):
        block = tq[:, n * qb:(n + 1) * qb].astype(F32) * scales[:, n:n + 1]
        XO[0, 2, lo:lo + rows, n * qb:(n + 1) * qb] = block.astype(BF16)

    pl.semaphore_wait(barrier, 31)

    def remote(src, dst, send, recv, who):
        c = pltpu.make_async_remote_copy(
            src_ref=src, dst_ref=dst, send_sem=send, recv_sem=recv, device_id=who, device_id_type=MESH
        )
        return c

    ag = {}
    leaving = {i: [] for i in range(4)}

    def gather_move(key, src_place, src, dst, who):
        n = len(ag)
        ag[key] = remote(src, dst, ag_send.at[n], ag_recv.at[n], who)
        leaving[PLACE[src_place][0]].append(ag[key])

    top, low = pl.ds(0, half), pl.ds(half, half)
    for name, part in (("t", top), ("l", low)):
        gather_move(("a", "3" + name), (0, 0), xin(0, 0).at[part, :], xin(0, 3).at[part, :], plus_a)
        gather_move(("a", "1" + name), (0, 0), xin(0, 0).at[part, :], xin(0, 1).at[part, :], minus_a)
    gather_move(("a", "2t"), (0, 3), xin(0, 3).at[top, :], xin(0, 2).at[top, :], plus_a)
    gather_move(("a", "2l"), (0, 1), xin(0, 1).at[low, :], xin(0, 2).at[low, :], minus_a)
    for da in range(4):
        gather_move((3, da), (0, da), xin(0, da), xin(3, da), plus_b)
        gather_move((1, da), (0, da), xin(0, da), xin(1, da), minus_b)
    for da in (0, 1):
        gather_move((2, da), (3, da), xin(3, da), xin(2, da), plus_b)
    for da in (3, 2):
        gather_move((2, da), (1, da), xin(1, da), xin(2, da), minus_b)
    dd = {}
    for c, (i, j) in PLACE.items():
        n = 4 * i + j
        dd[c] = remote(xin(*c), xin(*c, stream=1), dd_send.at[n], dd_recv.at[n], partner)
        leaving[i].append(dd[c])

    ag[("a", "3t")].start()
    ag[("a", "1l")].start()
    ag[("a", "3l")].start()
    ag[("a", "1t")].start()
    dd[(0, 0)].start()

    expert = lax.broadcasted_iota(jnp.int32, (32, rows), 0)
    gates = jnp.zeros((32, rows), F32)
    for k in range(ids.shape[0]):
        gates = gates + jnp.where(ids[k:k + 1, :] == expert, gv[k:k + 1, :], 0.0)
    before = (
        lax.broadcasted_iota(jnp.int32, (rows, rows), 0) < lax.broadcasted_iota(jnp.int32, (rows, rows), 1)
    ).astype(F32).astype(BF16)
    rank = dot((gates > 0.0).astype(F32).astype(BF16), before)
    TL[...] = jnp.zeros_like(TL)
    for e in range(32):
        TL[e, 0:1, 0:rows] = gates[e:e + 1, :]
        TL[e, 1:2, 0:rows] = rank[e:e + 1, :]
    tables = []
    for s in range(2):
        for (db, da), (i, j) in PLACE.items():
            n = 16 * s + 4 * i + j
            if n == 0:
                continue
            who = device(4 - da, 4 - db, s == 1)
            c = remote(TL.at[who["ep"]], T.at[n], t_send.at[n], t_recv.at[n], who)
            c.start()
            tables.append(c)
    T[0] = TL[ep]
    PF[...] = jnp.zeros_like(PF)

    def arrived(db, da):
        ag[(db, da)].wait_recv()
        if (db == 3 and da in (0, 1)) or (db == 1 and da in (3, 2)):
            ag[(2, da)].start()
        dd[(db, da)].start()

    def tables_of(i):
        slot = lax.broadcasted_iota(jnp.int32, (cap, 128), 0).astype(F32)
        for s in range(2):
            for j in range(4):
                t = T[16 * s + 4 * i + j]
                gate, place = t[0:1, :], t[1:2, :]
                pick = jnp.where((slot == place) & (gate > 0.0), 1.0, 0.0)
                weight = jnp.sum(pick * gate, axis=1, keepdims=True)
                GS[i, slots * s + cap * j:slots * s + cap * (j + 1), :] = jnp.broadcast_to(weight, (cap, 128))
                if rows == 64 and j % 2 == 1:
                    pick = pltpu.roll(pick, 64, 1)
                block = 128 * (rows * j // 128)
                PF[s, cap * j:cap * (j + 1), block:block + 128] = pick
            PB[i, s] = PF[s].astype(BF16)
            PT[i, s] = PF[s].T.astype(BF16)

    ag[("a", "3t")].wait_recv()
    ag[("a", "2t")].start()
    ag[("a", "1l")].wait_recv()
    ag[("a", "2l")].start()
    ag[(3, 0)].start()
    ag[(1, 0)].start()
    for c in tables:
        c.wait_recv()
    for i in range(2):
        tables_of(i)
    ag[("a", "1t")].wait_recv()
    ag[(3, 1)].start()
    ag[("a", "3l")].wait_recv()
    ag[(1, 3)].start()
    dd[(0, 1)].start()
    dd[(0, 3)].start()
    ag[("a", "2t")].wait_recv()
    ag[("a", "2l")].wait_recv()
    ag[(1, 2)].start()
    dd[(0, 2)].start()
    for i in range(2, 4):
        tables_of(i)
    arrived(3, 0)
    arrived(1, 0)
    ag[(3, 3)].start()

    wide = width // 2 if width % 256 == 0 else width

    def gather_rows(i, s):
        for n in range(width // wide):
            cols = slice(n * wide, (n + 1) * wide)
            XO[0, HOLD[i], slots * s:slots * (s + 1), cols] = dot(PB[i, s], XO[s, i + 2, :, cols]).astype(BF16)

    def gate_up(i):
        def products(n):
            cols = slice(n * htile, (n + 1) * htile)
            GU[n % 2, 0] = dot(XO[0, HOLD[i]], WG[:, cols])
            GU[n % 2, 1] = dot(XO[0, HOLD[i]], WU[:, cols])

        def activate(n):
            cols = slice(n * htile, (n + 1) * htile)
            g = GU[n % 2, 0]
            H[:, cols] = (g / (1.0 + jnp.exp(-g)) * GU[n % 2, 1]).astype(BF16)

        for n in range(hidden // htile):
            products(n)
            if n > 0:
                activate(n - 1)
        activate(hidden // htile - 1)

    def down(i):
        def part(n):
            cols = slice(n * tile, (n + 1) * tile)
            PV[n % 2] = (dot(H[...], WD[:, cols]) * GS[i, :, 0:1]).astype(BF16)

        def spread(n):
            cols = slice(n * tile, (n + 1) * tile)
            for s in range(2):
                XO[s, i, :, cols] = dot(PT[i, s], PV[n % 2, slots * s:slots * (s + 1)]).astype(BF16)

        for n in range(width // tile):
            part(n)
            if n > 0:
                spread(n - 1)
        spread(width // tile - 1)

    step_rows = 16

    def add_into(dst, *sources):
        def step(n, carry):
            r = pl.ds(pl.multiple_of(n * step_rows, step_rows), step_rows)
            total = dst[r, :].astype(F32)
            for src in sources:
                total = total + src[r, :].astype(F32)
            dst[r, :] = total.astype(BF16)
            return carry

        lax.fori_loop(0, dst.shape[0] // step_rows, step, 0)

    def part_of(db, da):
        i, j = PLACE[(db, da)]
        return S.at[i, pl.ds(rows * j, rows), :]

    swap = {}
    for c, (i, j) in PLACE.items():
        n = 4 * i + j
        src = XO.at[1, i, pl.ds(rows * j, rows), :]
        swap[c] = remote(src, part_of(*c), s_send.at[n], s_recv.at[n], partner)

    def merge(db, da, *more):
        swap[(db, da)].wait_recv()
        add_into(xout(db, da), part_of(db, da), *more)

    r1 = {}

    def r1_move(key, src, dst, who):
        n = len(r1)
        r1[key] = remote(src, dst, r1_send.at[n], r1_recv.at[n], who)

    far = ((2, 1), (0, 3))
    for n in range(2):
        r1_move(("f", 0, n), xout(2, far[0][n]), RF.at[0, n], plus_b)
        r1_move(("f", 1, n), xout(2, far[1][n]), RF.at[1, n], minus_b)
    for da in range(4):
        for sign, db, who in ((0, 1, plus_b), (1, 3, minus_b)):
            if (sign, da) in ((0, 1), (1, 3)):
                for part in ((low, top), (top, low))[sign]:
                    name = ("n", sign, da, "l" if part is low else "t")
                    r1_move(name, xout(db, da).at[part, :], RN.at[sign, da].at[part, :], who)
            else:
                r1_move(("n", sign, da), xout(db, da), RN.at[sign, da], who)

    def sent(i):
        for c in leaving[i]:
            c.wait_send()

    def pass_on(sign, n):
        db, da = (1, 3)[sign], far[sign][n]
        r1[("f", sign, n)].wait_recv()
        merge(db, da, RF.at[sign, n])
        r1[("n", sign, da)].start()

    def pass_on_halves(sign):
        db, da = (1, 3)[sign], far[sign][1]
        r1[("f", sign, 1)].wait_recv()
        swap[(db, da)].wait_recv()
        for name, part in ((("l", low), ("t", top)), (("t", top), ("l", low)))[sign]:
            add_into(xout(db, da).at[part, :], part_of(db, da).at[part, :], RF.at[sign, 1].at[part, :])
            r1[("n", sign, da, name)].start()

    def send_far(sign, n):
        merge(2, far[sign][n])
        r1[("f", sign, n)].start()

    def send_near(sign, da):
        merge((1, 3)[sign], da)
        r1[("n", sign, da)].start()

    for c in loads[:2]:
        c.wait()

    for i in range(4):
        for c in BATCHES[i]:
            dd[c].wait_recv()
        if i > 1:
            sent(i - 1)
        gather_rows(i, 0)
        gather_rows(i, 1)
        gate_up(i)
        if i == 0:
            loads[2].wait()
            arrived(3, 1)
            arrived(1, 3)
            ag[(3, 2)].start()
        elif i == 1:
            arrived(3, 3)
            arrived(2, 3)
        elif i == 2:
            arrived(3, 2)
            arrived(1, 1)
        elif i == 3:
            send_far(0, 0)
            send_far(1, 1)
            send_far(0, 1)
            pass_on(1, 0)
        if i == 2:
            sent(0)
        down(i)
        for c in BATCHES[i]:
            swap[c].start()
        if i == 0:
            arrived(1, 2)
            ag[(1, 1)].start()
            arrived(2, 0)
        elif i == 1:
            send_far(1, 0)
            send_near(0, 0)
            send_near(1, 1)
            send_near(0, 3)
            arrived(2, 1)
            arrived(2, 2)
    send_near(1, 2)
    pass_on(0, 0)
    pass_on_halves(1)
    pass_on_halves(0)

    def collect(da):
        r1[("n", 0, da)].wait_recv()
        r1[("n", 1, da)].wait_recv()
        merge(0, da, RN.at[0, da], RN.at[1, da])

    r2 = [
        remote(xout(0, 2).at[top, :], QF.at[0], r2_send.at[0], r2_recv.at[0], plus_a),
        remote(xout(0, 2).at[low, :], QF.at[1], r2_send.at[1], r2_recv.at[1], minus_a),
        remote(xout(0, 1).at[low, :], Q.at[0].at[low, :], r2_send.at[2], r2_recv.at[2], plus_a),
        remote(xout(0, 3).at[top, :], Q.at[1].at[top, :], r2_send.at[3], r2_recv.at[3], minus_a),
        remote(xout(0, 1).at[top, :], Q.at[0].at[top, :], r2_send.at[4], r2_recv.at[4], plus_a),
        remote(xout(0, 3).at[low, :], Q.at[1].at[low, :], r2_send.at[5], r2_recv.at[5], minus_a),
    ]
    collect(2)
    r2[0].start()
    r2[1].start()

    def collect_half(da, name, part, *more):
        sign = 0 if da == 1 else 1
        r1[("n", sign, da, name)].wait_recv()
        rest = [part_of(0, da), RN.at[0, da], RN.at[1, da]]
        add_into(xout(0, da).at[part, :], *[x.at[part, :] for x in rest], *more)

    swap[(0, 1)].wait_recv()
    swap[(0, 3)].wait_recv()
    r1[("n", 1, 1)].wait_recv()
    r1[("n", 0, 3)].wait_recv()
    collect_half(1, "l", low)
    r2[2].start()
    collect_half(3, "t", top)
    r2[3].start()
    r2[0].wait_recv()
    collect_half(1, "t", top, QF.at[0])
    r2[4].start()
    r2[1].wait_recv()
    collect_half(3, "l", low, QF.at[1])
    r2[5].start()

    r1[("n", 0, 0)].wait_recv()
    r1[("n", 1, 0)].wait_recv()
    mine, partners = xout(0, 0), part_of(0, 0)
    swap[(0, 0)].wait_recv()

    def start_sum(n, carry):
        r = pl.ds(pl.multiple_of(n * step_rows, step_rows), step_rows)
        mixed_out[r, :] = (
            res[r, :].astype(F32)
            + mine[r, :].astype(F32)
            + partners[r, :].astype(F32)
            + RN[0, 0, r, :].astype(F32)
            + RN[1, 0, r, :].astype(F32)
        )
        return carry

    lax.fori_loop(0, rows // step_rows, start_sum, 0)
    for n in (2, 3, 4, 5):
        r2[n].wait_recv()

    def finish(n, carry):
        r = pl.ds(pl.multiple_of(n * step_rows, step_rows), step_rows)
        mixed_out[r, :] = mixed_out[r, :] + Q[0, r, :].astype(F32) + Q[1, r, :].astype(F32)
        return carry

    lax.fori_loop(0, rows // step_rows, finish, 0)

    sent(3)
    for c in swap.values():
        c.wait_send()
    for c in tables:
        c.wait_send()
    for c in r1.values():
        c.wait_send()
    for c in r2:
        c.wait_send()


def norm_kernel(mixed_ref, gain, nr_out, nq_out, ns_out, SQ):
    rows, width = mixed_ref.shape
    qb = width // ns_out.shape[0]
    step_rows = 16
    SQ[...] = jnp.zeros_like(SQ)

    for n in range(rows // step_rows):
        r = slice(n * step_rows, (n + 1) * step_rows)
        mixed = mixed_ref[r, :]
        nr_out[r, :] = mixed.astype(BF16)
        scaled = lax.rsqrt(jnp.mean(mixed * mixed, axis=-1, keepdims=True) + 1e-06)
        lanes = lax.broadcasted_iota(jnp.int32, (step_rows, 128), 1)
        scales = jnp.zeros((step_rows, 128), F32)
        for b in range(width // qb):
            block = mixed[:, b * qb:(b + 1) * qb] * scaled * gain[b:b + 1, :]
            scale = (jnp.max(jnp.abs(block), axis=-1, keepdims=True) + 1e-06) / 448.0
            nq_out[r, b * qb:(b + 1) * qb] = (block * (1.0 / scale)).astype(BF16)
            scales = jnp.where(lanes == b, scale, scales)
        SQ[r, :] = scales
    ns_out[...] = SQ[...].T[0:width // qb, 0:rows]


def per_device(
    tokens_q, token_scale, residual, expert_ids, gate_values, w_gate, w_up, w_down, norm_gain
):
    rows, width = tokens_q.shape
    blocks = token_scale.shape[1]
    hidden = w_gate.shape[2]
    cap = rows // 2
    vmem = pl.BlockSpec(memory_space=pltpu.VMEM)
    hbm = pl.BlockSpec(memory_space=pl.ANY)
    dma = pltpu.SemaphoreType.DMA
    mixed = pl.pallas_call(
        functools.partial(kernel, cap),
        out_shape=jax.ShapeDtypeStruct((rows, width), F32),
        in_specs=[vmem] * 5 + [hbm] * 3,
        out_specs=vmem,
        scratch_shapes=[
            pltpu.VMEM((2, 6, 4 * rows, width), BF16),
            pltpu.VMEM((width, hidden), BF16),
            pltpu.VMEM((width, hidden), BF16),
            pltpu.VMEM((hidden, width), BF16),
            pltpu.VMEM((4, 4 * rows, width), BF16),
            pltpu.VMEM((2, 2, rows, width), BF16),
            pltpu.VMEM((2, 4, rows, width), BF16),
            pltpu.VMEM((2, rows // 2, width), BF16),
            pltpu.VMEM((2, rows, width), BF16),
            pltpu.VMEM((8 * cap, hidden), BF16),
            pltpu.VMEM((2, 2, 8 * cap, 256), F32),
            pltpu.VMEM((2, 8 * cap, tile_of(width)), BF16),
            pltpu.VMEM((2, 4 * cap, 4 * rows), F32),
            pltpu.VMEM((4, 2, 4 * cap, 4 * rows), BF16),
            pltpu.VMEM((4, 2, 4 * rows, 4 * cap), BF16),
            pltpu.VMEM((4, 8 * cap, 128), F32),
            pltpu.VMEM((32, 2, 128), F32),
            pltpu.VMEM((32, 2, 128), F32),
            pltpu.VMEM((128, 128), F32),
            dma((3,)), dma((32,)), dma((32,)), dma((18,)), dma((18,)), dma((16,)), dma((16,)),
            dma((16,)), dma((16,)), dma((14,)), dma((14,)), dma((6,)), dma((6,)),
        ],
        compiler_params=pltpu.CompilerParams(
            collective_id=0, has_side_effects=True, vmem_limit_bytes=67043328
        ),
    )(
        tokens_q, token_scale.T, residual, expert_ids.T, gate_values.T,
        w_gate[0], w_up[0], w_down[0],
    )
    new_residual, next_q, next_scale = pl.pallas_call(
        norm_kernel,
        out_shape=(
            jax.ShapeDtypeStruct((rows, width), BF16),
            jax.ShapeDtypeStruct((rows, width), BF16),
            jax.ShapeDtypeStruct((blocks, rows), F32),
        ),
        in_specs=[vmem] * 2,
        out_specs=(vmem, vmem, vmem),
        scratch_shapes=[pltpu.VMEM((128, 128), F32)],
    )(mixed, norm_gain.reshape(blocks, width // blocks))
    return new_residual, next_q, next_scale.T


def solution(mesh):
    rows = P(("dp", "ep"), None)
    weight = P("ep", None, None)
    return jax.shard_map(
        per_device,
        mesh=mesh,
        in_specs=(rows, rows, rows, rows, rows, weight, weight, weight, P()),
        out_specs=(rows, rows, rows),
        check_vma=False,
    )
```

```python
import functools

import jax
import jax.numpy as jnp
from jax import lax
from jax.experimental import pallas as pl
from jax.experimental.pallas import tpu as pltpu
from jax.sharding import PartitionSpec as P

MESH = pl.DeviceIdType.MESH
F32 = jnp.float32
BF16 = jnp.bfloat16

BATCHES = (
    ((0, 0), (0, 1), (0, 3), (0, 2)),
    ((2, 0), (1, 0), (3, 1), (1, 3)),
    ((2, 2), (2, 3), (2, 1), (3, 0)),
    ((3, 2), (1, 1), (1, 2), (3, 3)),
)
HOLD = (0, 1, 3, 4)
PLACE = {c: (i, j) for i, b in enumerate(BATCHES) for j, c in enumerate(b)}


def tile_of(width):
    return 896 if width % 896 == 0 else 256


def dot(a, b):
    return jnp.dot(a, b, preferred_element_type=F32)


def kernel(
    cap,
    tq, ts, res, ids, gv, wg_hbm, wu_hbm, wd_hbm,
    mixed_out,
    XO, WG, WU, WD, S, RF, RN, QF, Q, H, GU, PV, PF, PB, PT, GS, T, TL, SQ,
    w_sem, t_send, t_recv, ag_send, ag_recv, dd_send, dd_recv, s_send, s_recv, r1_send, r1_recv, r2_send, r2_recv,
):
    rows, width = tq.shape
    half = rows // 2
    hidden = wg_hbm.shape[1]
    qb = width // ts.shape[0]
    group = 4 * rows
    slots = 4 * cap
    tile = tile_of(width)
    htile = 256

    ep = lax.axis_index("ep")
    core = ep % 2
    z = (ep // 2) % 4
    y = ep // 8

    def device(da, db, other=False):
        yy = (y + da * (1 - core) + db * core) % 4
        zz = (z + da * core + db * (1 - core)) % 4
        cc = (1 - core) if other else core
        return {"ep": (yy * 4 + zz) * 2 + cc}

    plus_a, minus_a = device(1, 0), device(3, 0)
    plus_b, minus_b = device(0, 1), device(0, 3)
    partner = device(0, 0, True)

    barrier = pltpu.get_barrier_semaphore()

    def greet(k, carry):
        pl.semaphore_signal(barrier, inc=1, device_id={"ep": (ep + k) % 32}, device_id_type=MESH)
        return carry

    lax.fori_loop(1, 32, greet, 0)

    loads = [
        pltpu.make_async_copy(src, dst, w_sem.at[n])
        for n, (src, dst) in enumerate(((wg_hbm, WG), (wu_hbm, WU), (wd_hbm, WD)))
    ]
    for c in loads:
        c.start()

    def xin(db, da, stream=0):
        i, j = PLACE[(db, da)]
        return XO.at[stream, i + 2, pl.ds(rows * j, rows), :]

    def xout(db, da):
        i, j = PLACE[(db, da)]
        return XO.at[0, i, pl.ds(rows * j, rows), :]

    lo = rows * PLACE[(0, 0)][1]
    SQ[...] = jnp.zeros_like(SQ)
    SQ[0:width // qb, 0:rows] = ts[...]
    scales = SQ[...].T[0:rows]
    for n in range(width // qb):
        block = tq[:, n * qb:(n + 1) * qb].astype(F32) * scales[:, n:n + 1]
        XO[0, 2, lo:lo + rows, n * qb:(n + 1) * qb] = block.astype(BF16)

    pl.semaphore_wait(barrier, 31)

    def remote(src, dst, send, recv, who):
        c = pltpu.make_async_remote_copy(
            src_ref=src, dst_ref=dst, send_sem=send, recv_sem=recv, device_id=who, device_id_type=MESH
        )
        return c

    ag = {}
    leaving = {i: [] for i in range(4)}

    def gather_move(key, src_place, src, dst, who):
        n = len(ag)
        ag[key] = remote(src, dst, ag_send.at[n], ag_recv.at[n], who)
        leaving[PLACE[src_place][0]].append(ag[key])

    top, low = pl.ds(0, half), pl.ds(half, half)
    for name, part in (("t", top), ("l", low)):
        gather_move(("a", "3" + name), (0, 0), xin(0, 0).at[part, :], xin(0, 3).at[part, :], plus_a)
        gather_move(("a", "1" + name), (0, 0), xin(0, 0).at[part, :], xin(0, 1).at[part, :], minus_a)
    gather_move(("a", "2t"), (0, 3), xin(0, 3).at[top, :], xin(0, 2).at[top, :], plus_a)
    gather_move(("a", "2l"), (0, 1), xin(0, 1).at[low, :], xin(0, 2).at[low, :], minus_a)
    for da in range(4):
        gather_move((3, da), (0, da), xin(0, da), xin(3, da), plus_b)
        gather_move((1, da), (0, da), xin(0, da), xin(1, da), minus_b)
    for da in (0, 1):
        gather_move((2, da), (3, da), xin(3, da), xin(2, da), plus_b)
    for da in (3, 2):
        gather_move((2, da), (1, da), xin(1, da), xin(2, da), minus_b)
    dd = {}
    for c, (i, j) in PLACE.items():
        n = 4 * i + j
        dd[c] = remote(xin(*c), xin(*c, stream=1), dd_send.at[n], dd_recv.at[n], partner)
        leaving[i].append(dd[c])

    ag[("a", "3t")].start()
    ag[("a", "1l")].start()
    ag[("a", "3l")].start()
    ag[("a", "1t")].start()
    dd[(0, 0)].start()

    expert = lax.broadcasted_iota(jnp.int32, (32, rows), 0)
    gates = jnp.zeros((32, rows), F32)
    for k in range(ids.shape[0]):
        gates = gates + jnp.where(ids[k:k + 1, :] == expert, gv[k:k + 1, :], 0.0)
    before = (
        lax.broadcasted_iota(jnp.int32, (rows, rows), 0) < lax.broadcasted_iota(jnp.int32, (rows, rows), 1)
    ).astype(F32).astype(BF16)
    rank = dot((gates > 0.0).astype(F32).astype(BF16), before)
    TL[...] = jnp.zeros_like(TL)
    for e in range(32):
        TL[e, 0:1, 0:rows] = gates[e:e + 1, :]
        TL[e, 1:2, 0:rows] = rank[e:e + 1, :]
    tables = []
    for s in range(2):
        for (db, da), (i, j) in PLACE.items():
            n = 16 * s + 4 * i + j
            if n == 0:
                continue
            who = device(4 - da, 4 - db, s == 1)
            c = remote(TL.at[who["ep"]], T.at[n], t_send.at[n], t_recv.at[n], who)
            c.start()
            tables.append(c)
    T[0] = TL[ep]
    PF[...] = jnp.zeros_like(PF)

    def arrived(db, da):
        ag[(db, da)].wait_recv()
        if (db == 3 and da in (0, 1)) or (db == 1 and da in (3, 2)):
            ag[(2, da)].start()
        dd[(db, da)].start()

    def tables_of(i):
        slot = lax.broadcasted_iota(jnp.int32, (cap, 128), 0).astype(F32)
        for s in range(2):
            for j in range(4):
                t = T[16 * s + 4 * i + j]
                gate, place = t[0:1, :], t[1:2, :]
                pick = jnp.where((slot == place) & (gate > 0.0), 1.0, 0.0)
                weight = jnp.sum(pick * gate, axis=1, keepdims=True)
                GS[i, slots * s + cap * j:slots * s + cap * (j + 1), :] = jnp.broadcast_to(weight, (cap, 128))
                if rows == 64 and j % 2 == 1:
                    pick = pltpu.roll(pick, 64, 1)
                block = 128 * (rows * j // 128)
                PF[s, cap * j:cap * (j + 1), block:block + 128] = pick
            PB[i, s] = PF[s].astype(BF16)
            PT[i, s] = PF[s].T.astype(BF16)

    ag[("a", "3t")].wait_recv()
    ag[("a", "2t")].start()
    ag[("a", "1l")].wait_recv()
    ag[("a", "2l")].start()
    ag[(3, 0)].start()
    ag[(1, 0)].start()
    for c in tables:
        c.wait_recv()
    for i in range(2):
        tables_of(i)
    ag[("a", "1t")].wait_recv()
    ag[(3, 1)].start()
    ag[("a", "3l")].wait_recv()
    ag[(1, 3)].start()
    dd[(0, 1)].start()
    dd[(0, 3)].start()
    ag[("a", "2t")].wait_recv()
    ag[("a", "2l")].wait_recv()
    ag[(1, 2)].start()
    dd[(0, 2)].start()
    for i in range(2, 4):
        tables_of(i)
    arrived(3, 0)
    arrived(1, 0)
    ag[(3, 3)].start()

    wide = width // 2 if width % 256 == 0 else width

    def gather_rows(i, s):
        for n in range(width // wide):
            cols = slice(n * wide, (n + 1) * wide)
            XO[0, HOLD[i], slots * s:slots * (s + 1), cols] = dot(PB[i, s], XO[s, i + 2, :, cols]).astype(BF16)

    def gate_up(i):
        def products(n):
            cols = slice(n * htile, (n + 1) * htile)
            GU[n % 2, 0] = dot(XO[0, HOLD[i]], WG[:, cols])
            GU[n % 2, 1] = dot(XO[0, HOLD[i]], WU[:, cols])

        def activate(n):
            cols = slice(n * htile, (n + 1) * htile)
            g = GU[n % 2, 0]
            H[:, cols] = (g / (1.0 + jnp.exp(-g)) * GU[n % 2, 1]).astype(BF16)

        for n in range(hidden // htile):
            products(n)
            if n > 0:
                activate(n - 1)
        activate(hidden // htile - 1)

    def down(i):
        def part(n):
            cols = slice(n * tile, (n + 1) * tile)
            PV[n % 2] = (dot(H[...], WD[:, cols]) * GS[i, :, 0:1]).astype(BF16)

        def spread(n):
            cols = slice(n * tile, (n + 1) * tile)
            for s in range(2):
                XO[s, i, :, cols] = dot(PT[i, s], PV[n % 2, slots * s:slots * (s + 1)]).astype(BF16)

        for n in range(width // tile):
            part(n)
            if n > 0:
                spread(n - 1)
        spread(width // tile - 1)

    step_rows = 16

    def add_into(dst, *sources):
        def step(n, carry):
            r = pl.ds(pl.multiple_of(n * step_rows, step_rows), step_rows)
            total = dst[r, :].astype(F32)
            for src in sources:
                total = total + src[r, :].astype(F32)
            dst[r, :] = total.astype(BF16)
            return carry

        lax.fori_loop(0, dst.shape[0] // step_rows, step, 0)

    def part_of(db, da):
        i, j = PLACE[(db, da)]
        return S.at[i, pl.ds(rows * j, rows), :]

    swap = {}
    for c, (i, j) in PLACE.items():
        n = 4 * i + j
        src = XO.at[1, i, pl.ds(rows * j, rows), :]
        swap[c] = remote(src, part_of(*c), s_send.at[n], s_recv.at[n], partner)

    def merge(db, da, *more):
        swap[(db, da)].wait_recv()
        add_into(xout(db, da), part_of(db, da), *more)

    r1 = {}

    def r1_move(key, src, dst, who):
        n = len(r1)
        r1[key] = remote(src, dst, r1_send.at[n], r1_recv.at[n], who)

    far = ((2, 1), (0, 3))
    for n in range(2):
        r1_move(("f", 0, n), xout(2, far[0][n]), RF.at[0, n], plus_b)
        r1_move(("f", 1, n), xout(2, far[1][n]), RF.at[1, n], minus_b)
    for da in range(4):
        for sign, db, who in ((0, 1, plus_b), (1, 3, minus_b)):
            if (sign, da) in ((0, 1), (1, 3)):
                for part in ((low, top), (top, low))[sign]:
                    name = ("n", sign, da, "l" if part is low else "t")
                    r1_move(name, xout(db, da).at[part, :], RN.at[sign, da].at[part, :], who)
            else:
                r1_move(("n", sign, da), xout(db, da), RN.at[sign, da], who)

    def sent(i):
        for c in leaving[i]:
            c.wait_send()

    def pass_on(sign, n):
        db, da = (1, 3)[sign], far[sign][n]
        r1[("f", sign, n)].wait_recv()
        merge(db, da, RF.at[sign, n])
        r1[("n", sign, da)].start()

    def pass_on_halves(sign):
        db, da = (1, 3)[sign], far[sign][1]
        r1[("f", sign, 1)].wait_recv()
        swap[(db, da)].wait_recv()
        for name, part in ((("l", low), ("t", top)), (("t", top), ("l", low)))[sign]:
            add_into(xout(db, da).at[part, :], part_of(db, da).at[part, :], RF.at[sign, 1].at[part, :])
            r1[("n", sign, da, name)].start()

    def send_far(sign, n):
        merge(2, far[sign][n])
        r1[("f", sign, n)].start()

    def send_near(sign, da):
        merge((1, 3)[sign], da)
        r1[("n", sign, da)].start()

    for c in loads[:2]:
        c.wait()

    for i in range(4):
        for c in BATCHES[i]:
            dd[c].wait_recv()
        if i > 1:
            sent(i - 1)
        gather_rows(i, 0)
        gather_rows(i, 1)
        gate_up(i)
        if i == 0:
            loads[2].wait()
            arrived(3, 1)
            arrived(1, 3)
            ag[(3, 2)].start()
        elif i == 1:
            arrived(3, 3)
            arrived(2, 3)
        elif i == 2:
            arrived(3, 2)
            arrived(1, 1)
        elif i == 3:
            send_far(0, 0)
            send_far(1, 1)
            send_far(0, 1)
            pass_on(1, 0)
        if i == 2:
            sent(0)
        down(i)
        for c in BATCHES[i]:
            swap[c].start()
        if i == 0:
            arrived(1, 2)
            ag[(1, 1)].start()
            arrived(2, 0)
        elif i == 1:
            arrived(2, 1)
            arrived(2, 2)
            send_far(1, 0)
            send_near(0, 0)
            send_near(1, 1)
            send_near(0, 3)
    send_near(1, 2)
    pass_on(0, 0)
    pass_on_halves(1)
    pass_on_halves(0)

    def collect(da):
        r1[("n", 0, da)].wait_recv()
        r1[("n", 1, da)].wait_recv()
        merge(0, da, RN.at[0, da], RN.at[1, da])

    r2 = [
        remote(xout(0, 2).at[top, :], QF.at[0], r2_send.at[0], r2_recv.at[0], plus_a),
        remote(xout(0, 2).at[low, :], QF.at[1], r2_send.at[1], r2_recv.at[1], minus_a),
        remote(xout(0, 1).at[low, :], Q.at[0].at[low, :], r2_send.at[2], r2_recv.at[2], plus_a),
        remote(xout(0, 3).at[top, :], Q.at[1].at[top, :], r2_send.at[3], r2_recv.at[3], minus_a),
        remote(xout(0, 1).at[top, :], Q.at[0].at[top, :], r2_send.at[4], r2_recv.at[4], plus_a),
        remote(xout(0, 3).at[low, :], Q.at[1].at[low, :], r2_send.at[5], r2_recv.at[5], minus_a),
    ]
    collect(2)
    r2[0].start()
    r2[1].start()

    def collect_half(da, name, part, *more):
        sign = 0 if da == 1 else 1
        r1[("n", sign, da, name)].wait_recv()
        rest = [part_of(0, da), RN.at[0, da], RN.at[1, da]]
        add_into(xout(0, da).at[part, :], *[x.at[part, :] for x in rest], *more)

    swap[(0, 1)].wait_recv()
    swap[(0, 3)].wait_recv()
    r1[("n", 1, 1)].wait_recv()
    r1[("n", 0, 3)].wait_recv()
    collect_half(1, "l", low)
    r2[2].start()
    collect_half(3, "t", top)
    r2[3].start()
    r2[0].wait_recv()
    collect_half(1, "t", top, QF.at[0])
    r2[4].start()
    r2[1].wait_recv()
    collect_half(3, "l", low, QF.at[1])
    r2[5].start()

    r1[("n", 0, 0)].wait_recv()
    r1[("n", 1, 0)].wait_recv()
    mine, partners = xout(0, 0), part_of(0, 0)
    swap[(0, 0)].wait_recv()

    def start_sum(n, carry):
        r = pl.ds(pl.multiple_of(n * step_rows, step_rows), step_rows)
        mixed_out[r, :] = (
            res[r, :].astype(F32)
            + mine[r, :].astype(F32)
            + partners[r, :].astype(F32)
            + RN[0, 0, r, :].astype(F32)
            + RN[1, 0, r, :].astype(F32)
        )
        return carry

    lax.fori_loop(0, rows // step_rows, start_sum, 0)
    for n in (2, 3, 4, 5):
        r2[n].wait_recv()

    def finish(n, carry):
        r = pl.ds(pl.multiple_of(n * step_rows, step_rows), step_rows)
        mixed_out[r, :] = mixed_out[r, :] + Q[0, r, :].astype(F32) + Q[1, r, :].astype(F32)
        return carry

    lax.fori_loop(0, rows // step_rows, finish, 0)

    sent(3)
    for c in swap.values():
        c.wait_send()
    for c in tables:
        c.wait_send()
    for c in r1.values():
        c.wait_send()
    for c in r2:
        c.wait_send()


def norm_kernel(mixed_ref, gain, nr_out, nq_out, ns_out, SQ):
    rows, width = mixed_ref.shape
    qb = width // ns_out.shape[0]
    step_rows = 16
    SQ[...] = jnp.zeros_like(SQ)

    for n in range(rows // step_rows):
        r = slice(n * step_rows, (n + 1) * step_rows)
        mixed = mixed_ref[r, :]
        nr_out[r, :] = mixed.astype(BF16)
        scaled = lax.rsqrt(jnp.mean(mixed * mixed, axis=-1, keepdims=True) + 1e-06)
        lanes = lax.broadcasted_iota(jnp.int32, (step_rows, 128), 1)
        scales = jnp.zeros((step_rows, 128), F32)
        for b in range(width // qb):
            block = mixed[:, b * qb:(b + 1) * qb] * scaled * gain[b:b + 1, :]
            scale = (jnp.max(jnp.abs(block), axis=-1, keepdims=True) + 1e-06) / 448.0
            nq_out[r, b * qb:(b + 1) * qb] = (block * (1.0 / scale)).astype(BF16)
            scales = jnp.where(lanes == b, scale, scales)
        SQ[r, :] = scales
    ns_out[...] = SQ[...].T[0:width // qb, 0:rows]


def per_device(
    tokens_q, token_scale, residual, expert_ids, gate_values, w_gate, w_up, w_down, norm_gain
):
    rows, width = tokens_q.shape
    blocks = token_scale.shape[1]
    hidden = w_gate.shape[2]
    cap = rows // 2
    vmem = pl.BlockSpec(memory_space=pltpu.VMEM)
    hbm = pl.BlockSpec(memory_space=pl.ANY)
    dma = pltpu.SemaphoreType.DMA
    mixed = pl.pallas_call(
        functools.partial(kernel, cap),
        out_shape=jax.ShapeDtypeStruct((rows, width), F32),
        in_specs=[vmem] * 5 + [hbm] * 3,
        out_specs=vmem,
        scratch_shapes=[
            pltpu.VMEM((2, 6, 4 * rows, width), BF16),
            pltpu.VMEM((width, hidden), BF16),
            pltpu.VMEM((width, hidden), BF16),
            pltpu.VMEM((hidden, width), BF16),
            pltpu.VMEM((4, 4 * rows, width), BF16),
            pltpu.VMEM((2, 2, rows, width), BF16),
            pltpu.VMEM((2, 4, rows, width), BF16),
            pltpu.VMEM((2, rows // 2, width), BF16),
            pltpu.VMEM((2, rows, width), BF16),
            pltpu.VMEM((8 * cap, hidden), BF16),
            pltpu.VMEM((2, 2, 8 * cap, 256), F32),
            pltpu.VMEM((2, 8 * cap, tile_of(width)), BF16),
            pltpu.VMEM((2, 4 * cap, 4 * rows), F32),
            pltpu.VMEM((4, 2, 4 * cap, 4 * rows), BF16),
            pltpu.VMEM((4, 2, 4 * rows, 4 * cap), BF16),
            pltpu.VMEM((4, 8 * cap, 128), F32),
            pltpu.VMEM((32, 2, 128), F32),
            pltpu.VMEM((32, 2, 128), F32),
            pltpu.VMEM((128, 128), F32),
            dma((3,)), dma((32,)), dma((32,)), dma((18,)), dma((18,)), dma((16,)), dma((16,)),
            dma((16,)), dma((16,)), dma((14,)), dma((14,)), dma((6,)), dma((6,)),
        ],
        compiler_params=pltpu.CompilerParams(
            collective_id=0, has_side_effects=True, vmem_limit_bytes=67043328
        ),
    )(
        tokens_q, token_scale.T, residual, expert_ids.T, gate_values.T,
        w_gate[0], w_up[0], w_down[0],
    )
    new_residual, next_q, next_scale = pl.pallas_call(
        norm_kernel,
        out_shape=(
            jax.ShapeDtypeStruct((rows, width), BF16),
            jax.ShapeDtypeStruct((rows, width), BF16),
            jax.ShapeDtypeStruct((blocks, rows), F32),
        ),
        in_specs=[vmem] * 2,
        out_specs=(vmem, vmem, vmem),
        scratch_shapes=[pltpu.VMEM((128, 128), F32)],
    )(mixed, norm_gain.reshape(blocks, width // blocks))
    return new_residual, next_q, next_scale.T


def solution(mesh):
    rows = P(("dp", "ep"), None)
    weight = P("ep", None, None)
    return jax.shard_map(
        per_device,
        mesh=mesh,
        in_specs=(rows, rows, rows, rows, rows, weight, weight, weight, P()),
        out_specs=(rows, rows, rows),
        check_vma=False,
    )
```
